256 devices in a mesh: layer: 4 (over y), row: 8 (over x, core), col: 8 (over z).
Axes of the slice: x: 4, y: 4, z: 8, core: 2. Of those that a mesh axis runs over, the one named last changes fastest.
Arguments:
- hidden: bfloat16 [1536, 2304], P(('layer', 'row')), may hold values from -60 to 60
- embedding: bfloat16 [131072, 2304], P(('row', 'col'), 'layer'), may hold values from -0.3 to 0.3
- teacher: bfloat16 [1536, 131072], P('layer', ('row', 'col')), may hold values from -80 to 240
Outputs:
- grad_embedding: float32 [131072, 2304], P(('row', 'col'), 'layer')
- grad_hidden: float32 [1536, 2304], P(('layer', 'row', 'col'))
The draws below stay inside these ranges and needn't reach their ends.
All inputs are finite; a program needn't handle non-finite values.
Results may differ from the reference program's by a relative error of at most 0.0041.
Values may be sent and summed in bfloat16 or wider, within the bound.
No kernel may reach another device: no remote copies, remote signals or barrier semaphores. Data moves between devices by JAX's collectives and lax.ppermute only.
A program may use at most 192 MiB of HBM per device.

```python
import math
import jax
import jax.numpy as jnp
from jax import lax

D = 2304
LOSS_SCALE = 256
TOKENS = 1536
VOCAB = 131072


def embed_row(base_key, index):
    row_key = jax.random.fold_in(base_key, index)
    values = jnp.clip(jax.random.normal(row_key, (D,), jnp.float32), -6.0, 6.0) * D ** (-0.5)
    factor = 1.0 + 0.1 * index.astype(jnp.float32) / VOCAB
    bound = 14.4 * D ** (-0.5)
    return jnp.clip(values * factor, -bound, bound)


def embed_table(key):
    base_key = jax.random.fold_in(key, 11)
    return jax.vmap(lambda index: embed_row(base_key, index))(jnp.arange(VOCAB, dtype=jnp.int32))


def draw_embedding(key, part):
    return embed_table(key).astype(jnp.bfloat16)


def draw_hidden(key, part):
    drawn = jnp.clip(jax.random.normal(jax.random.fold_in(key, 21), (TOKENS, D), jnp.float32), -6.0, 6.0) * 3.0
    bound = 2880.0 * D ** (-0.5)
    return jnp.clip(drawn, -bound, bound).astype(jnp.bfloat16)


def draw_teacher(key, part):
    noise = jnp.clip(jax.random.normal(jax.random.fold_in(key, 41), (TOKENS, VOCAB), jnp.float32), -6.0, 6.0)
    rising = jnp.log(3.0) * jnp.arange(VOCAB, dtype=jnp.float32)[None, :] / VOCAB
    values = noise * 3.0 + rising
    return values.astype(jnp.bfloat16)


def setup_inputs(seed: int = 0) -> dict:
    streams_of = jax.random.split(jax.random.key(seed), 4)
    hidden = draw_hidden(jax.random.fold_in(streams_of[3], 71), 0)
    embedding = draw_embedding(jax.random.fold_in(streams_of[3], 71), 0)
    teacher = draw_teacher(jax.random.fold_in(streams_of[3], 71), 0)
    return dict(hidden=hidden, embedding=embedding, teacher=teacher)


def reference(hidden, embedding, teacher):
    tokens = hidden.shape[0]
    block = math.gcd(tokens, 256)
    nblocks = tokens // block
    hid_blocks = hidden.reshape(nblocks, block, hidden.shape[1])
    tea_blocks = teacher.reshape(nblocks, block, teacher.shape[1])

    def one_block(acc_embed, pair):
        hid_part, tea_part = pair
        logits = lax.dot_general(hid_part, embedding, (((1,), (1,)), ((), ())), preferred_element_type=jnp.float32)
        teach_f = tea_part.astype(jnp.float32)
        top_s = jnp.max(logits, axis=1)
        top_t = jnp.max(teach_f, axis=1)
        sum_s = jnp.sum(jnp.exp(logits - top_s[:, None]), axis=1)
        sum_t = jnp.sum(jnp.exp(teach_f - top_t[:, None]), axis=1)
        lse_s = top_s + jnp.log(sum_s)
        lse_t = top_t + jnp.log(sum_t)
        prob_s = jnp.exp(logits - lse_s[:, None])
        prob_t = jnp.exp(teach_f - lse_t[:, None])
        grads = ((prob_s - prob_t) * LOSS_SCALE).astype(jnp.bfloat16)
        grad_hid = jnp.dot(grads, embedding, preferred_element_type=jnp.float32)
        acc_embed = acc_embed + lax.dot_general(grads, hid_part, (((0,), (0,)), ((), ())), preferred_element_type=jnp.float32)
        return acc_embed, grad_hid

    start_acc = jnp.zeros(embedding.shape, jnp.float32)
    grad_embedding, grad_hid = lax.scan(one_block, start_acc, (hid_blocks, tea_blocks))
    return grad_embedding, grad_hid.reshape(tokens, hidden.shape[1])
```

```python
import jax
import jax.numpy as jnp
from jax import lax
from jax.sharding import PartitionSpec as P

LOSS_SCALE = 256


def shift_y(x, s):
    n = lax.axis_size("layer")
    return lax.ppermute(x, "layer", [(i, (i + s) % n) for i in range(n)])


def shift_x(x, s):
    n = lax.axis_size("row")
    return lax.ppermute(x, "row", [(i, (i + 2 * s) % n) for i in range(n)])


def shift_z(x, s):
    n = lax.axis_size("col")
    return lax.ppermute(x, "col", [(i, (i + s) % n) for i in range(n)])


def swap_core(x):
    n = lax.axis_size("row")
    return lax.ppermute(x, "row", [(i, i ^ 1) for i in range(n)])


def at(x, k, dim=0):
    return lax.dynamic_index_in_dim(x, k, dim, keepdims=False)


def put(buf, x, k, dim=0):
    return lax.dynamic_update_slice_in_dim(buf, jnp.expand_dims(x, dim), k, dim)


def ring_gather(block, shift):
    half = block.shape[0] // 2
    back = shift(block, 1)
    front = shift(block, -1)
    far = (shift(back[:half], 1), shift(front[half:], -1))
    return ((0, block), (3, back), (1, front), (2, jnp.concatenate(far)))


def ring_exchange(piece, shift):
    far = piece(2)
    half = far.shape[0] // 2
    right, left = shift(far[:half], 1), shift(far[half:], -1)
    back = shift(piece(1), 1)
    front = shift(piece(3), -1)
    far = (shift(right, 1), shift(left, -1))
    return ((0, piece(0)), (3, back), (1, front), (2, jnp.concatenate(far)))


def ring_sum(piece, shift):
    f32, bf16 = jnp.float32, jnp.bfloat16
    far = piece(2)
    half = far.shape[0] // 2
    right, left = shift(far[:half], 1), shift(far[half:], -1)
    ahead, behind = piece(1), piece(3)
    back_b = shift(ahead[half:], 1)
    front_a = shift(behind[:half], -1)
    back_a = shift((ahead[:half].astype(f32) + right.astype(f32)).astype(bf16), 1)
    front_b = shift((behind[half:].astype(f32) + left.astype(f32)).astype(bf16), -1)
    own = piece(0).astype(f32)
    first = own[:half] + back_a.astype(f32) + front_a.astype(f32)
    second = own[half:] + back_b.astype(f32) + front_b.astype(f32)
    return jnp.concatenate([first, second])


def joined(parts):
    top_s = parts[0][0]
    top_t = parts[0][2]
    for p in parts[1:]:
        top_s = jnp.maximum(top_s, p[0])
        top_t = jnp.maximum(top_t, p[2])
    sum_s = sum(p[1] * jnp.exp(p[0] - top_s) for p in parts)
    sum_t = sum(p[3] * jnp.exp(p[2] - top_t) for p in parts)
    return jnp.stack([top_s, sum_s, top_t, sum_t])


def local(hidden, embedding, teacher):
    f32, bf16 = jnp.float32, jnp.bfloat16
    layers, cols = lax.axis_size("layer"), lax.axis_size("col")
    xs = lax.axis_size("row") // 2
    y = lax.axis_index("layer")
    row = lax.axis_index("row")
    x, core = row // 2, row % 2
    strip, width = hidden.shape
    quarter = embedding.shape[1]
    block = embedding.shape[0] // layers
    tokens = strip * layers * xs * 2

    table = embedding.T
    pieces = ring_exchange(
        lambda k: lax.dynamic_slice_in_dim(table, ((y + k) % layers) * block, block, 1), shift_y
    )
    table = jnp.zeros((layers, quarter, block), bf16)
    for k, p in pieces:
        table = put(table, p, (y + k) % layers)
    table = table.reshape(width, block)

    mine = jnp.zeros((layers, strip, width), bf16)
    for k, p in ring_gather(hidden, shift_y):
        mine = put(mine, p, (y + k) % layers)
    held = jnp.zeros((xs, layers * strip, width), bf16)
    for k, p in ring_gather(mine.reshape(layers * strip, width), shift_x):
        held = put(held, p, (x + k) % xs)
    states = jnp.zeros((2, tokens // 2, width), bf16)
    held = held.reshape(tokens // 2, width)
    states = put(states, held, core)
    states = put(states, swap_core(held), 1 - core)
    states = states.reshape(tokens, width)

    pieces = ring_exchange(
        lambda k: lax.dynamic_slice_in_dim(teacher, ((y + k) % layers) * block, block, 1), shift_y
    )
    taught = jnp.zeros((2, xs, layers, strip, block), bf16)
    for k, p in pieces:
        p = p.reshape(xs, 2, strip, block).swapaxes(0, 1)
        taught = put(taught, p, (y + k) % layers, 2)
    taught = taught.reshape(tokens, block).astype(f32)

    logits = jnp.dot(states, table, preferred_element_type=f32)
    top_s = jnp.max(logits, axis=1)
    top_t = jnp.max(taught, axis=1)
    sum_s = jnp.sum(jnp.exp(logits - top_s[:, None]), axis=1)
    sum_t = jnp.sum(jnp.exp(taught - top_t[:, None]), axis=1)
    stats = jnp.stack([top_s, sum_s, top_t, sum_t])
    stats = joined([stats, swap_core(stats)])
    stats = joined([stats] + [shift_x(stats, k) for k in range(1, xs)])
    stats = joined([stats] + [shift_y(stats, k) for k in range(1, layers)])
    stats = joined([stats] + [shift_z(stats, k) for k in range(1, cols)])
    lse_s = stats[0] + jnp.log(stats[1])
    lse_t = stats[2] + jnp.log(stats[3])
    prob_s = jnp.exp(logits - lse_s[:, None])
    prob_t = jnp.exp(taught - lse_t[:, None])
    grads = ((prob_s - prob_t) * LOSS_SCALE).astype(bf16)

    halves = grads.reshape(2, tokens // 2, block)
    both = jnp.concatenate([at(halves, core), swap_core(at(halves, 1 - core))], axis=1)
    both = both.reshape(xs, layers * strip, 2 * block)
    tables = jnp.concatenate([table, swap_core(table)], axis=1)

    def part(k):
        rows = at(both, (x + k) % xs)
        return lax.dot_general(
            rows, tables, (((1,), (1,)), ((), ())), preferred_element_type=f32
        ).astype(bf16)

    summed = ring_sum(part, shift_x).astype(bf16)
    summed = summed.reshape(layers, cols, strip // cols, width).swapaxes(0, 1)
    summed = lax.all_to_all(summed, "col", 0, 0, tiled=True)
    summed = jnp.sum(summed.astype(f32), axis=0).astype(bf16)
    summed = lax.all_to_all(summed, "layer", 0, 0, tiled=True)
    grad_hidden = jnp.sum(summed.astype(f32), axis=0)

    grad_table = lax.dot_general(
        states, grads, (((0,), (0,)), ((), ())), preferred_element_type=f32
    ).astype(bf16)
    grad_table = grad_table.reshape(layers, quarter, block)
    pieces = ring_exchange(lambda k: at(grad_table, (y + k) % layers), shift_y)
    grad_embedding = jnp.zeros((quarter, layers * block), f32)
    for k, p in pieces:
        grad_embedding = lax.dynamic_update_slice_in_dim(
            grad_embedding, p.astype(f32), ((y + k) % layers) * block, 1
        )
    return grad_embedding.T, grad_hidden


def solution(mesh):
    placed = (P(("layer", "row"), None), P(("row", "col"), "layer"), P("layer", ("row", "col")))
    return jax.shard_map(
        local,
        mesh=mesh,
        in_specs=placed,
        out_specs=(P(("row", "col"), "layer"), P(("layer", "row", "col"), None)),
        check_vma=False,
    )
```

```python
import jax
import jax.numpy as jnp
from jax import lax
from jax.sharding import PartitionSpec as P

LOSS_SCALE = 256

def shift_x(x, s):
    n = lax.axis_size("row")
    return lax.ppermute(x, "row", [(i, (i + 2 * s) % n) for i in range(n)])

def swap_core(x):
    n = lax.axis_size("row")
    return lax.ppermute(x, "row", [(i, i ^ 1) for i in range(n)])

def at(x, k, dim=0):
    return lax.dynamic_index_in_dim(x, k, dim, keepdims=False)

def put(buf, x, k, dim=0):
    return lax.dynamic_update_slice_in_dim(buf, jnp.expand_dims(x, dim), k, dim)

def ring_gather(block, shift):
    half = block.shape[0] // 2
    back = shift(block, 1)
    front = shift(block, -1)
    far = (shift(back[:half], 1), shift(front[half:], -1))
    return ((0, block), (3, back), (1, front), (2, jnp.concatenate(far)))

def ring_sum(piece, shift):
    f32, bf16 = jnp.float32, jnp.bfloat16
    far = piece(2)
    half = far.shape[0] // 2
    right, left = shift(far[:half], 1), shift(far[half:], -1)
    ahead, behind = piece(1), piece(3)
    back_b = shift(ahead[half:], 1)
    front_a = shift(behind[:half], -1)
    back_a = shift((ahead[:half].astype(f32) + right.astype(f32)).astype(bf16), 1)
    front_b = shift((behind[half:].astype(f32) + left.astype(f32)).astype(bf16), -1)
    own = piece(0).astype(f32)
    first = own[:half] + back_a.astype(f32) + front_a.astype(f32)
    second = own[half:] + back_b.astype(f32) + front_b.astype(f32)
    return jnp.concatenate([first, second])

def spread(x, axis):
    n = lax.axis_size(axis)
    return lax.all_to_all(jnp.broadcast_to(x[None], (n, *x.shape)), axis, 0, 0, tiled=True)

def joined(top, total, dim):
    best = jnp.max(top, axis=dim)
    scale = jnp.exp(top - jnp.expand_dims(best, dim))
    return best, jnp.sum(total * scale, axis=dim)

def local(hidden, embedding, teacher):
    f32, bf16 = jnp.float32, jnp.bfloat16
    layers, cols = lax.axis_size("layer"), lax.axis_size("col")
    rows = lax.axis_size("row")
    xs = rows // 2
    row = lax.axis_index("row")
    x, core = row // 2, row % 2
    strip, width = hidden.shape
    quarter = embedding.shape[1]
    block = embedding.shape[0] // layers
    home = strip * rows
    tokens = home * layers

    mine = spread(hidden, "layer")
    held = jnp.zeros((layers, xs, strip, width), bf16)
    for k, p in ring_gather(mine.reshape(layers * strip, width), shift_x):
        held = put(held, p.reshape(layers, strip, width), (x + k) % xs, 1)
    states = jnp.zeros((layers, xs, 2, strip, width), bf16)
    states = put(states, held, core, 2)
    states = put(states, swap_core(held), 1 - core, 2)
    states = states.reshape(tokens, width)

    table = embedding.T.reshape(quarter, layers, block).swapaxes(0, 1)
    table = lax.all_to_all(table, "layer", 0, 0, tiled=True).reshape(width, block)

    taught = teacher.reshape(home, layers, block).swapaxes(0, 1)
    taught = lax.all_to_all(taught, "layer", 0, 0, tiled=True)
    taught = taught.reshape(tokens, block).astype(f32)

    home_f = teacher.astype(f32)
    top_t = jnp.max(home_f, axis=1)
    sum_t = jnp.sum(jnp.exp(home_f - top_t[:, None]), axis=1)
    logits = jnp.dot(states, table, preferred_element_type=f32)
    top_s = jnp.max(logits, axis=1)
    sum_s = jnp.sum(jnp.exp(logits - top_s[:, None]), axis=1)
    stats = jnp.stack([jnp.concatenate([top_s, top_t]), jnp.concatenate([sum_s, sum_t])])
    got = spread(stats, ("layer", "row"))
    top_s, sum_s = joined(got[:, 0, :tokens], got[:, 1, :tokens], 0)
    got = got[:, :, tokens:].reshape(layers, rows, 2, home)
    top_t, sum_t = joined(got[:, :, 0], got[:, :, 1], 1)
    stats = jnp.stack([top_s, sum_s, top_t.reshape(tokens), sum_t.reshape(tokens)])
    got = spread(stats, "col")
    top_s, sum_s = joined(got[:, 0], got[:, 1], 0)
    top_t, sum_t = joined(got[:, 2], got[:, 3], 0)
    lse_s = top_s + jnp.log(sum_s)
    lse_t = top_t + jnp.log(sum_t)
    prob_s = jnp.exp(logits - lse_s[:, None])
    prob_t = jnp.exp(taught - lse_t[:, None])
    grads = ((prob_s - prob_t) * LOSS_SCALE).astype(bf16)

    halves = grads.reshape(layers, xs, 2, strip, block)
    half = lambda c: at(halves, c, 2).swapaxes(0, 1).reshape(tokens // 2, block)
    both = jnp.concatenate([half(core), swap_core(half(1 - core))], axis=1)
    both = both.reshape(xs, layers * strip, 2 * block)
    tables = jnp.concatenate([table, swap_core(table)], axis=1)

    def part(k):
        lines = at(both, (x + k) % xs)
        return lax.dot_general(
            lines, tables, (((1,), (1,)), ((), ())), preferred_element_type=f32
        ).astype(bf16)

    parts = {k: part(k) for k in (2, 1, 3)}
    grads, parts = lax.optimization_barrier((grads, parts))
    parts[0] = part(0)
    summed = ring_sum(lambda k: parts[k], shift_x).astype(bf16)
    summed = summed.reshape(layers * cols, strip // cols, width)
    summed = lax.all_to_all(summed, ("layer", "col"), 0, 0, tiled=True)
    grad_hidden = jnp.sum(summed.astype(f32), axis=0)

    grad_table = lax.dot_general(
        states, grads, (((0,), (0,)), ((), ())), preferred_element_type=f32
    ).astype(bf16)
    grad_table = grad_table.reshape(layers, quarter, block)
    grad_table = lax.all_to_all(grad_table, "layer", 0, 0, tiled=True)
    grad_table = grad_table.astype(f32).swapaxes(0, 1).reshape(quarter, layers * block)
    return grad_table.T, grad_hidden


def solution(mesh):
    placed = (P(("layer", "row"), None), P(("row", "col"), "layer"), P("layer", ("row", "col")))
    return jax.shard_map(
        local,
        mesh=mesh,
        in_specs=placed,
        out_specs=(P(("row", "col"), "layer"), P(("layer", "row", "col"), None)),
        check_vma=False,
    )
```

```python
import jax
import jax.numpy as jnp
from jax import lax
from jax.sharding import PartitionSpec as P

LOSS_SCALE = 256


def shift_y(x, s):
    n = lax.axis_size("layer")
    return lax.ppermute(x, "layer", [(i, (i + s) % n) for i in range(n)])


def shift_x(x, s):
    n = lax.axis_size("row")
    return lax.ppermute(x, "row", [(i, (i + 2 * s) % n) for i in range(n)])


def swap_core(x):
    n = lax.axis_size("row")
    return lax.ppermute(x, "row", [(i, i ^ 1) for i in range(n)])


def at(x, k, dim=0):
    return lax.dynamic_index_in_dim(x, k, dim, keepdims=False)


def put(buf, x, k, dim=0):
    return lax.dynamic_update_slice_in_dim(buf, jnp.expand_dims(x, dim), k, dim)


def ring_gather(block, shift):
    half = block.shape[0] // 2
    back = shift(block, 1)
    front = shift(block, -1)
    far = (shift(back[:half], 1), shift(front[half:], -1))
    return ((0, block), (3, back), (1, front), (2, jnp.concatenate(far)))


def ring_sum_far(far, shift):
    half = far.shape[0] // 2
    return shift(far[:half], 1), shift(far[half:], -1)


def ring_sum(own, ahead, behind, far, shift):
    right, left = far
    none = jnp.zeros_like(right)
    back = shift(ahead + jnp.concatenate([right, none]), 1)
    front = shift(behind + jnp.concatenate([none, left]), -1)
    f32 = jnp.float32
    return own.astype(f32) + back.astype(f32) + front.astype(f32)


def spread(x, axis):
    n = lax.axis_size(axis)
    return lax.all_to_all(jnp.broadcast_to(x[None], (n, *x.shape)), axis, 0, 0, tiled=True)


def logsum(values, dim):
    top = jnp.max(values, axis=dim)
    return top + jnp.log(jnp.sum(jnp.exp(values - jnp.expand_dims(top, dim)), axis=dim))


def ordered(core, own, other):
    return jnp.where(core == 0, jnp.stack([own, other]), jnp.stack([other, own]))


def local(hidden, embedding, teacher):
    f32, bf16 = jnp.float32, jnp.bfloat16
    layers, cols = lax.axis_size("layer"), lax.axis_size("col")
    rows = lax.axis_size("row")
    xs = rows // 2
    y, row = lax.axis_index("layer"), lax.axis_index("row")
    x, core = row // 2, row % 2
    strip, width = hidden.shape
    quarter = embedding.shape[1]
    block = embedding.shape[0] // layers
    half = strip * xs * layers

    moved = [shift_y(hidden, k) for k in (1, 3, 2)]
    mine = jnp.zeros((layers, strip, width), bf16)
    for k, p in ((0, hidden), (3, moved[0]), (1, moved[1]), (2, moved[2])):
        mine = put(mine, p, (y + k) % layers)

    table = embedding.T
    table = jnp.stack([table[:, k * block : (k + 1) * block] for k in range(layers)])
    table = lax.all_to_all(table, "layer", 0, 0, tiled=True).reshape(width, block)

    taught = jnp.stack([teacher[:, k * block : (k + 1) * block] for k in range(layers)])
    taught = lax.all_to_all(taught, "layer", 0, 0, tiled=True)
    taught = taught.reshape(layers, xs, 2, strip, block)

    own = jnp.zeros((xs, layers * strip, width), bf16)
    pieces = ring_gather(mine.reshape(layers * strip, width), shift_x)
    for k, p in pieces:
        own = put(own, p, (x + k) % xs)
    own = own.reshape(half, width)
    other = swap_core(own)

    side = lambda c: at(taught, c, 2).swapaxes(0, 1).reshape(half, block).astype(f32)
    taught_own, taught_other = side(core), side(1 - core)
    logits_own = jnp.dot(own, table, preferred_element_type=f32)
    logits_other = jnp.dot(other, table, preferred_element_type=f32)
    lse = ordered(
        core,
        jnp.stack([logsum(logits_own, 1), logsum(taught_own, 1)]),
        jnp.stack([logsum(logits_other, 1), logsum(taught_other, 1)]),
    )
    lse = lse.reshape(2, 2, xs, layers, strip).transpose(3, 2, 0, 1, 4)
    got = lax.all_to_all(lse.reshape(layers * rows, 2 * strip), ("layer", "row"), 0, 0, tiled=True)
    lse = logsum(got, 0)
    got = spread(lse, ("layer", "row", "col"))
    lse = logsum(got.reshape(layers * rows, cols, 2 * strip), 1)
    lse = lse.reshape(layers, xs, 2, 2, strip).transpose(2, 3, 1, 0, 4).reshape(2, 2, half)

    def gradient(logits, taught, lse):
        prob_s = jnp.exp(logits - lse[0][:, None])
        prob_t = jnp.exp(taught - lse[1][:, None])
        return ((prob_s - prob_t) * LOSS_SCALE).astype(bf16)

    grads_other = gradient(logits_other, taught_other, at(lse, 1 - core))
    crossed = swap_core(grads_other)
    grads_own = gradient(logits_own, taught_own, at(lse, core))
    other_table = swap_core(table)

    both = jnp.concatenate([grads_own, crossed], axis=1).reshape(xs, layers * strip, 2 * block)
    tables = jnp.concatenate([table, other_table], axis=1)

    def part(k):
        lines = at(both, (x + k) % xs)
        return lax.dot_general(
            lines, tables, (((1,), (1,)), ((), ())), preferred_element_type=f32
        ).astype(bf16)

    grads = jnp.concatenate([grads_own, grads_other])
    states = jnp.concatenate([own, other])
    far = ring_sum_far(part(2), shift_x)
    grad_table = lax.dot_general(
        states, grads, (((0,), (0,)), ((), ())), preferred_element_type=f32
    ).astype(bf16)
    both, grad_table = lax.optimization_barrier((both, grad_table))
    grad_table = grad_table.reshape(layers, quarter, block)
    grad_table = lax.all_to_all(grad_table, "layer", 0, 0, tiled=True)
    grad_table = jnp.concatenate([grad_table[k].astype(f32) for k in range(layers)], axis=1)

    near = part(1), part(3)
    both, near = lax.optimization_barrier((both, near))
    summed = ring_sum(lax.optimization_barrier(part(0)), *near, far, shift_x).astype(bf16)
    summed = summed.reshape(layers, strip, width)
    summed = lax.all_to_all(summed, "layer", 0, 0, tiled=True)
    summed = jnp.sum(summed.astype(f32), axis=0).astype(bf16)
    summed = summed.reshape(cols, strip // cols, width)
    summed = lax.all_to_all(summed, "col", 0, 0, tiled=True)
    grad_hidden = jnp.sum(summed.astype(f32), axis=0)
    return grad_table.T, grad_hidden


def solution(mesh):
    placed = (P(("layer", "row"), None), P(("row", "col"), "layer"), P("layer", ("row", "col")))
    return jax.shard_map(
        local,
        mesh=mesh,
        in_specs=placed,
        out_specs=(P(("row", "col"), "layer"), P(("layer", "row", "col"), None)),
        check_vma=False,
    )
```

```python
import jax
import jax.numpy as jnp
from jax import lax
from jax.sharding import PartitionSpec as P

LOSS_SCALE = 256


def shift_y(x, s):
    n = lax.axis_size("layer")
    return lax.ppermute(x, "layer", [(i, (i + s) % n) for i in range(n)])


def shift_x(x, s):
    n = lax.axis_size("row")
    return lax.ppermute(x, "row", [(i, (i + 2 * s) % n) for i in range(n)])


def swap_core(x):
    n = lax.axis_size("row")
    return lax.ppermute(x, "row", [(i, i ^ 1) for i in range(n)])


def at(x, k, dim=0):
    return lax.dynamic_index_in_dim(x, k, dim, keepdims=False)


def put(buf, x, k, dim=0):
    return lax.dynamic_update_slice_in_dim(buf, jnp.expand_dims(x, dim), k, dim)


def ring_gather(block, shift):
    half = block.shape[0] // 2
    back = shift(block, 1)
    front = shift(block, -1)
    far = (shift(back[:half], 1), shift(front[half:], -1))
    return ((0, block), (3, back), (1, front), (2, jnp.concatenate(far)))


def ring_sum_far(far, shift):
    half = far.shape[0] // 2
    return shift(far[:half], 1), shift(far[half:], -1)


def ring_sum(own, ahead, behind, far, shift):
    right, left = far
    none = jnp.zeros_like(right)
    back = shift(ahead + jnp.concatenate([right, none]), 1)
    front = shift(behind + jnp.concatenate([none, left]), -1)
    f32 = jnp.float32
    return own.astype(f32) + back.astype(f32) + front.astype(f32)


def spread(x, axis):
    n = lax.axis_size(axis)
    return lax.all_to_all(jnp.broadcast_to(x[None], (n, *x.shape)), axis, 0, 0, tiled=True)


def logsum(values, dim):
    top = jnp.max(values, axis=dim)
    return top + jnp.log(jnp.sum(jnp.exp(values - jnp.expand_dims(top, dim)), axis=dim))


def ordered(core, own, other):
    return jnp.where(core == 0, jnp.stack([own, other]), jnp.stack([other, own]))


def local(hidden, embedding, teacher):
    f32, bf16 = jnp.float32, jnp.bfloat16
    layers, cols = lax.axis_size("layer"), lax.axis_size("col")
    rows = lax.axis_size("row")
    xs = rows // 2
    y, row = lax.axis_index("layer"), lax.axis_index("row")
    x, core = row // 2, row % 2
    strip, width = hidden.shape
    quarter = embedding.shape[1]
    block = embedding.shape[0] // layers
    half = strip * xs * layers

    moved = [shift_y(hidden, k) for k in (1, 3, 2)]
    mine = jnp.zeros((layers, strip, width), bf16)
    for k, p in ((0, hidden), (3, moved[0]), (1, moved[1]), (2, moved[2])):
        mine = put(mine, p, (y + k) % layers)

    table = embedding.T
    cut = lambda m, k: m[:, k * block : (k + 1) * block]
    sent = [jnp.concatenate([cut(table, k), cut(teacher, k)]) for k in range(layers)]
    sent = lax.all_to_all(jnp.stack(sent), "layer", 0, 0, tiled=True)
    table = sent[:, :quarter].reshape(width, block)
    taught = sent[:, quarter:].reshape(layers, xs, 2, strip, block)

    own = jnp.zeros((xs, layers * strip, width), bf16)
    pieces = ring_gather(mine.reshape(layers * strip, width), shift_x)
    for k, p in pieces:
        own = put(own, p, (x + k) % xs)
    own = own.reshape(half, width)
    other = swap_core(own)

    states = jnp.concatenate([own, other])
    logits = jnp.dot(states, table, preferred_element_type=f32)
    lse_s = logsum(logits, 1)
    lse_s = ordered(core, lse_s[:half], lse_s[half:])
    lse_t = logsum(teacher.astype(f32), 1)
    got = spread(jnp.concatenate([lse_s.reshape(2 * half), lse_t]), ("layer", "row"))
    lse_s = logsum(got[:, : 2 * half], 0)
    lse_t = logsum(got[:, 2 * half :].reshape(layers, rows, -1), 1)
    got = spread(jnp.concatenate([lse_s, lse_t.reshape(2 * half)]), "col")
    lse_s, lse_t = jnp.split(logsum(got, 0), 2)
    lse_s = lse_s.reshape(2, half)
    lse_t = lse_t.reshape(layers, xs, 2, strip).transpose(2, 1, 0, 3).reshape(2, half)

    def gradient(logits, c):
        taught_c = at(taught, c, 2).swapaxes(0, 1).reshape(half, block).astype(f32)
        prob_s = jnp.exp(logits - at(lse_s, c)[:, None])
        prob_t = jnp.exp(taught_c - at(lse_t, c)[:, None])
        return ((prob_s - prob_t) * LOSS_SCALE).astype(bf16)

    grads_other = gradient(logits[half:], 1 - core)
    crossed = swap_core(grads_other)
    grads_own = gradient(logits[:half], core)
    other_table = swap_core(table)

    both = jnp.concatenate([grads_own, crossed], axis=1).reshape(xs, layers * strip, 2 * block)
    tables = jnp.concatenate([table, other_table], axis=1)

    def part(*ks):
        lines = jnp.concatenate([at(both, (x + k) % xs) for k in ks])
        return lax.dot_general(
            lines, tables, (((1,), (1,)), ((), ())), preferred_element_type=f32
        ).astype(bf16)

    grads = jnp.concatenate([grads_own, grads_other])
    far = ring_sum_far(part(2), shift_x)
    grad_table = lax.dot_general(
        states, grads, (((0,), (0,)), ((), ())), preferred_element_type=f32
    ).astype(bf16)
    both, grad_table = lax.optimization_barrier((both, grad_table))
    grad_table = grad_table.reshape(layers, quarter, block)
    grad_table = lax.all_to_all(grad_table, "layer", 0, 0, tiled=True)
    grad_table = jnp.concatenate([grad_table[k].astype(f32) for k in range(layers)], axis=1)

    ahead, behind, here = jnp.split(lax.optimization_barrier(part(1, 3, 0)), 3)
    summed = ring_sum(here, ahead, behind, far, shift_x).astype(bf16)
    summed = summed.reshape(layers, strip, width)
    summed = lax.all_to_all(summed, "layer", 0, 0, tiled=True)
    summed = jnp.sum(summed.astype(f32), axis=0).astype(bf16)
    summed = summed.reshape(cols, strip // cols, width)
    summed = lax.all_to_all(summed, "col", 0, 0, tiled=True)
    grad_hidden = jnp.sum(summed.astype(f32), axis=0)
    return grad_table.T, grad_hidden


def solution(mesh):
    placed = (P(("layer", "row"), None), P(("row", "col"), "layer"), P("layer", ("row", "col")))
    return jax.shard_map(
        local,
        mesh=mesh,
        in_specs=placed,
        out_specs=(P(("row", "col"), "layer"), P(("layer", "row", "col"), None)),
        check_vma=False,
    )
```

```python
import jax
import jax.numpy as jnp
from jax import lax
from jax.experimental import pallas as pl
from jax.sharding import PartitionSpec as P

LOSS_SCALE = 256


def shift_y(x, s):
    n = lax.axis_size("layer")
    return lax.ppermute(x, "layer", [(i, (i + s) % n) for i in range(n)])


def shift_x(x, s):
    n = lax.axis_size("row")
    return lax.ppermute(x, "row", [(i, (i + 2 * s) % n) for i in range(n)])


def swap_core(x):
    n = lax.axis_size("row")
    return lax.ppermute(x, "row", [(i, i ^ 1) for i in range(n)])


def at(x, k, dim=0):
    return lax.dynamic_index_in_dim(x, k, dim, keepdims=False)


def put(buf, x, k, dim=0):
    return lax.dynamic_update_slice_in_dim(buf, jnp.expand_dims(x, dim), k, dim)


def ring_gather(block, shift):
    half = block.shape[0] // 2
    back = shift(block, 1)
    front = shift(block, -1)
    far = (shift(back[:half], 1), shift(front[half:], -1))
    return ((0, block), (3, back), (1, front), (2, jnp.concatenate(far)))


def ring_sum_far(far, shift):
    half = far.shape[0] // 2
    return shift(far[:half], 1), shift(far[half:], -1)


def ring_sum(own, ahead, behind, far, shift):
    right, left = far
    none = jnp.zeros_like(right)
    back = shift(ahead + jnp.concatenate([right, none]), 1)
    front = shift(behind + jnp.concatenate([none, left]), -1)
    f32 = jnp.float32
    return own.astype(f32) + back.astype(f32) + front.astype(f32)


def spread(x, axis):
    n = lax.axis_size(axis)
    return lax.all_to_all(jnp.broadcast_to(x[None], (n, *x.shape)), axis, 0, 0, tiled=True)


def logsum(values, dim):
    top = jnp.max(values, axis=dim)
    return top + jnp.log(jnp.sum(jnp.exp(values - jnp.expand_dims(top, dim)), axis=dim))


def whole(x):
    return pl.BlockSpec(x.shape, lambda i: (0,) * x.ndim)


def cost(rows, depth, cols, moved):
    return pl.CostEstimate(flops=2 * rows * depth * cols, bytes_accessed=moved, transcendentals=0)


def scores_kernel(state_ref, table_ref, out_ref, sum_ref):
    out = jnp.dot(state_ref[...], table_ref[...], preferred_element_type=jnp.float32)
    out_ref[...] = out
    top = jnp.max(out, axis=1, keepdims=True)
    total = top + jnp.log(jnp.sum(jnp.exp(out - top), axis=1, keepdims=True))
    total = jnp.broadcast_to(total, (out.shape[0], 128)).T
    sum_ref[...] = total[: sum_ref.shape[0]]


def scores(states, table):
    tokens, width = states.shape
    block = table.shape[1]
    tile = 256 if tokens % 256 == 0 else tokens
    logits, sums = pl.pallas_call(
        scores_kernel,
        grid=(tokens // tile,),
        in_specs=[pl.BlockSpec((tile, width), lambda i: (i, 0)), whole(table)],
        out_specs=[
            pl.BlockSpec((tile, block), lambda i: (i, 0)),
            pl.BlockSpec((8, tile), lambda i: (0, i)),
        ],
        out_shape=[
            jax.ShapeDtypeStruct((tokens, block), jnp.float32),
            jax.ShapeDtypeStruct((8, tokens), jnp.float32),
        ],
        cost_estimate=cost(tokens, width, block, 2 * tokens * width + 4 * tokens * block),
    )(states, table)
    return logits, sums[0]


def part_kernel(mine_ref, other_ref, table_ref, far_ref, out_ref):
    over = (((1,), (1,)), ((), ()))
    f32 = jnp.float32
    total = lax.dot_general(mine_ref[...], table_ref[...], over, preferred_element_type=f32)
    total += lax.dot_general(other_ref[...], far_ref[...], over, preferred_element_type=f32)
    out_ref[...] = total.astype(out_ref.dtype)


def part_of(mine, other, table, far):
    tokens, block = mine.shape
    width = table.shape[0]
    tile = 384 if width % 384 == 0 else width
    band = pl.BlockSpec((tile, block), lambda i: (i, 0))
    return pl.pallas_call(
        part_kernel,
        grid=(width // tile,),
        in_specs=[whole(mine), whole(other), band, band],
        out_specs=pl.BlockSpec((tokens, tile), lambda i: (0, i)),
        out_shape=jax.ShapeDtypeStruct((tokens, width), jnp.bfloat16),
        cost_estimate=cost(tokens, 2 * block, width, 4 * width * block),
    )(mine, other, table, far)


def table_kernel(own_ref, other_ref, own_grad_ref, other_grad_ref, out_ref):
    over = (((0,), (0,)), ((), ()))
    f32 = jnp.float32
    total = lax.dot_general(own_ref[...], own_grad_ref[...], over, preferred_element_type=f32)
    total += lax.dot_general(other_ref[...], other_grad_ref[...], over, preferred_element_type=f32)
    out_ref[...] = total.astype(out_ref.dtype)


def table_gradient(own, other, own_grads, other_grads):
    tokens, width = own.shape
    block = own_grads.shape[1]
    tile = 256 if width % 256 == 0 else width
    band = pl.BlockSpec((tokens, tile), lambda i: (0, i))
    return pl.pallas_call(
        table_kernel,
        grid=(width // tile,),
        in_specs=[band, band, whole(own_grads), whole(other_grads)],
        out_specs=pl.BlockSpec((tile, block), lambda i: (i, 0)),
        out_shape=jax.ShapeDtypeStruct((width, block), jnp.bfloat16),
        cost_estimate=cost(2 * tokens, width, block, 4 * tokens * width),
    )(own, other, own_grads, other_grads)


def ordered(core, own, other):
    return jnp.where(core == 0, jnp.stack([own, other]), jnp.stack([other, own]))


def local(hidden, embedding, teacher):
    f32, bf16 = jnp.float32, jnp.bfloat16
    layers, cols = lax.axis_size("layer"), lax.axis_size("col")
    rows = lax.axis_size("row")
    xs = rows // 2
    y, row = lax.axis_index("layer"), lax.axis_index("row")
    x, core = row // 2, row % 2
    strip, width = hidden.shape
    quarter = embedding.shape[1]
    block = embedding.shape[0] // layers
    half = strip * xs * layers

    moved = [shift_y(hidden, k) for k in (1, 3, 2)]
    mine = jnp.zeros((layers, strip, width), bf16)
    for k, p in ((0, hidden), (3, moved[0]), (1, moved[1]), (2, moved[2])):
        mine = put(mine, p, (y + k) % layers)

    table = embedding.T
    cut = lambda m, k: m[:, k * block : (k + 1) * block]
    sent = [jnp.concatenate([cut(table, k), cut(teacher, k)]) for k in range(layers)]
    sent = lax.all_to_all(jnp.stack(sent), "layer", 0, 0, tiled=True)
    table = sent[:, :quarter].reshape(width, block)
    taught = sent[:, quarter:].reshape(layers, xs, 2, strip, block)

    own = jnp.zeros((layers, xs, strip, width), bf16)
    pieces = ring_gather(mine.reshape(layers * strip, width), shift_x)
    for k, p in pieces:
        own = put(own, p.reshape(layers, strip, width), (x + k) % xs, 1)
    own = own.reshape(half, width)
    other = swap_core(own)

    logits_own, sum_own = scores(own, table)
    logits_other, sum_other = scores(other, table)
    lse_s = ordered(core, sum_own, sum_other)
    lse_t = logsum(teacher.astype(f32), 1)
    got = spread(jnp.concatenate([lse_s.reshape(2 * half), lse_t]), ("layer", "row"))
    lse_s = logsum(got[:, : 2 * half], 0)
    lse_t = logsum(got[:, 2 * half :].reshape(layers, rows, -1), 1)
    got = spread(jnp.concatenate([lse_s, lse_t.reshape(2 * half)]), "col")
    lse_s, lse_t = jnp.split(logsum(got, 0), 2)
    lse_s = lse_s.reshape(2, half)
    lse_t = lse_t.reshape(layers * xs, 2, strip).swapaxes(0, 1).reshape(2, half)

    def gradient(logits, c):
        taught_c = at(taught, c, 2).reshape(half, block).astype(f32)
        prob_s = jnp.exp(logits - at(lse_s, c)[:, None])
        prob_t = jnp.exp(taught_c - at(lse_t, c)[:, None])
        return ((prob_s - prob_t) * LOSS_SCALE).astype(bf16)

    grads_other = gradient(logits_other, 1 - core)
    crossed = swap_core(grads_other)
    grads_own = gradient(logits_own, core)
    other_table = swap_core(table)


    def part(*ks):
        def lines(grads):
            grads = grads.reshape(layers, xs, strip, block)
            picked = [at(grads, (x + k) % xs, 1).reshape(layers * strip, block) for k in ks]
            return jnp.concatenate(picked)

        return part_of(lines(grads_own), lines(crossed), table, other_table)

    far = ring_sum_far(part(2), shift_x)

    grad_table = table_gradient(own, other, grads_own, grads_other)
    crossed, grad_table = lax.optimization_barrier((crossed, grad_table))
    grad_table = grad_table.reshape(layers, quarter, block)
    grad_table = lax.all_to_all(grad_table, "layer", 0, 0, tiled=True)
    grad_table = jnp.concatenate([grad_table[k].astype(f32) for k in range(layers)], axis=1)

    ahead, behind, here = jnp.split(part(1, 3, 0), 3)
    summed = ring_sum(here, ahead, behind, far, shift_x).astype(bf16)
    summed = summed.reshape(layers, strip, width)
    summed = lax.all_to_all(summed, "layer", 0, 0, tiled=True)
    summed = jnp.sum(summed.astype(f32), axis=0).astype(bf16)
    summed = summed.reshape(cols, strip // cols, width)
    summed = lax.all_to_all(summed, "col", 0, 0, tiled=True)
    grad_hidden = jnp.sum(summed.astype(f32), axis=0)
    return grad_table.T, grad_hidden


def solution(mesh):
    placed = (P(("layer", "row"), None), P(("row", "col"), "layer"), P("layer", ("row", "col")))
    return jax.shard_map(
        local,
        mesh=mesh,
        in_specs=placed,
        out_specs=(P(("row", "col"), "layer"), P(("layer", "row", "col"), None)),
        check_vma=False,
    )
```

```python
import jax
import jax.numpy as jnp
from jax import lax
from jax.experimental.layout import Layout, with_layout_constraint
from jax.sharding import PartitionSpec as P

LOSS_SCALE = 256


def shift_y(x, s):
    n = lax.axis_size("layer")
    return lax.ppermute(x, "layer", [(i, (i + s) % n) for i in range(n)])


def shift_x(x, s):
    n = lax.axis_size("row")
    return lax.ppermute(x, "row", [(i, (i + 2 * s) % n) for i in range(n)])


def swap_core(x):
    n = lax.axis_size("row")
    return lax.ppermute(x, "row", [(i, i ^ 1) for i in range(n)])


def at(x, k, dim=0):
    return lax.dynamic_index_in_dim(x, k, dim, keepdims=False)


def put(buf, x, k, dim=0):
    return lax.dynamic_update_slice_in_dim(buf, jnp.expand_dims(x, dim), k, dim)


def ring_gather(block, shift):
    half = block.shape[0] // 2
    back = shift(block, 1)
    front = shift(block, -1)
    far = (shift(back[:half], 1), shift(front[half:], -1))
    return ((0, block), (3, back), (1, front), (2, jnp.concatenate(far)))


def ring_sum_far(far, shift):
    half = far.shape[0] // 2
    return shift(far[:half], 1), shift(far[half:], -1)


def ring_sum(own, ahead, behind, far, shift):
    right, left = far
    none = jnp.zeros_like(right)
    back = shift(ahead + jnp.concatenate([right, none]), 1)
    front = shift(behind + jnp.concatenate([none, left]), -1)
    f32 = jnp.float32
    return own.astype(f32) + back.astype(f32) + front.astype(f32)


def spread(x, axis):
    n = lax.axis_size(axis)
    return lax.all_to_all(jnp.broadcast_to(x[None], (n, *x.shape)), axis, 0, 0, tiled=True)


def logsum(values, dim):
    top = jnp.max(values, axis=dim)
    return top + jnp.log(jnp.sum(jnp.exp(values - jnp.expand_dims(top, dim)), axis=dim))


def ordered(core, own, other):
    return jnp.where(core == 0, jnp.stack([own, other]), jnp.stack([other, own]))


def local(hidden, embedding, teacher):
    f32, bf16 = jnp.float32, jnp.bfloat16
    layers, cols = lax.axis_size("layer"), lax.axis_size("col")
    rows = lax.axis_size("row")
    xs = rows // 2
    y, row = lax.axis_index("layer"), lax.axis_index("row")
    x, core = row // 2, row % 2
    strip, width = hidden.shape
    quarter = embedding.shape[1]
    block = embedding.shape[0] // layers
    half = strip * xs * layers

    moved = [shift_y(hidden, k) for k in (1, 3, 2)]
    mine = jnp.zeros((layers, strip, width), bf16)
    for k, p in ((0, hidden), (3, moved[0]), (1, moved[1]), (2, moved[2])):
        mine = put(mine, p, (y + k) % layers)

    table = embedding.T
    cut = lambda m, k: m[:, k * block : (k + 1) * block]
    sent = [jnp.concatenate([cut(table, k), cut(teacher, k)]) for k in range(layers)]
    sent = lax.all_to_all(jnp.stack(sent), "layer", 0, 0, tiled=True)
    table = sent[:, :quarter].reshape(width, block)
    taught = sent[:, quarter:].reshape(layers, xs, 2, strip, block)
    taught = [at(taught, c, 2).reshape(half, block) for c in (core, 1 - core)]

    own = jnp.zeros((layers, xs, strip, width), bf16)
    pieces = ring_gather(mine.reshape(layers * strip, width), shift_x)
    for k, p in pieces:
        own = put(own, p.reshape(layers, strip, width), (x + k) % xs, 1)
    own = own.reshape(half, width)
    other = swap_core(own)

    states = jnp.concatenate([own, other])
    logits = jnp.dot(states, table, preferred_element_type=f32)
    logits = with_layout_constraint(logits, Layout((0, 1)))
    lse_s = logsum(logits, 1)
    lse_s = ordered(core, lse_s[:half], lse_s[half:])
    lse_t = logsum(teacher.astype(f32), 1)
    got = spread(jnp.concatenate([lse_s.reshape(2 * half), lse_t]), ("layer", "row"))
    lse_s = logsum(got[:, : 2 * half], 0)
    lse_t = logsum(got[:, 2 * half :].reshape(layers, rows, -1), 1)
    got = spread(jnp.concatenate([lse_s, lse_t.reshape(2 * half)]), "col")
    lse_s, lse_t = jnp.split(logsum(got, 0), 2)
    lse_s = lse_s.reshape(2, half)
    lse_t = lse_t.reshape(layers * xs, 2, strip).swapaxes(0, 1).reshape(2, half)

    def gradient(logits, taught_c, c):
        taught_c = taught_c.astype(f32)
        prob_s = jnp.exp(logits - at(lse_s, c)[:, None])
        prob_t = jnp.exp(taught_c - at(lse_t, c)[:, None])
        return ((prob_s - prob_t) * LOSS_SCALE).astype(bf16)

    grads_other = gradient(logits[half:], taught[1], 1 - core)
    crossed = swap_core(grads_other)
    grads_own = gradient(logits[:half], taught[0], core)
    other_table = swap_core(table)


    both = jnp.concatenate([grads_own, crossed], axis=1)
    both = both.reshape(layers, xs, strip, 2 * block)
    tables = jnp.concatenate([table, other_table], axis=1)

    def part(*ks):
        picked = [at(both, (x + k) % xs, 1).reshape(layers * strip, 2 * block) for k in ks]
        return lax.dot_general(
            jnp.concatenate(picked), tables, (((1,), (1,)), ((), ())), preferred_element_type=f32
        ).astype(bf16)

    far = ring_sum_far(part(2), shift_x)

    grads = jnp.concatenate([grads_own, grads_other])
    grad_table = lax.dot_general(
        states, grads, (((0,), (0,)), ((), ())), preferred_element_type=f32
    ).astype(bf16)
    both, grad_table = lax.optimization_barrier((both, grad_table))
    grad_table = grad_table.reshape(layers, quarter, block)
    grad_table = lax.all_to_all(grad_table, "layer", 0, 0, tiled=True)
    grad_table = jnp.concatenate([grad_table[k].astype(f32) for k in range(layers)], axis=1)

    ahead, behind, here = jnp.split(lax.optimization_barrier(part(1, 3, 0)), 3)
    summed = ring_sum(here, ahead, behind, far, shift_x).astype(bf16)
    summed = summed.reshape(layers * cols, strip // cols, width)
    summed = lax.all_to_all(summed, ("layer", "col"), 0, 0, tiled=True)
    grad_hidden = jnp.sum(summed.astype(f32), axis=0)
    return grad_table.T, grad_hidden


def solution(mesh):
    placed = (P(("layer", "row"), None), P(("row", "col"), "layer"), P("layer", ("row", "col")))
    return jax.shard_map(
        local,
        mesh=mesh,
        in_specs=placed,
        out_specs=(P(("row", "col"), "layer"), P(("layer", "row", "col"), None)),
        check_vma=False,
    )
```

```python
import jax
import jax.numpy as jnp
from jax import lax
from jax.experimental.layout import Layout, with_layout_constraint
from jax.sharding import PartitionSpec as P

LOSS_SCALE = 256


def shift_y(x, s):
    n = lax.axis_size("layer")
    return lax.ppermute(x, "layer", [(i, (i + s) % n) for i in range(n)])


def shift_x(x, s):
    n = lax.axis_size("row")
    return lax.ppermute(x, "row", [(i, (i + 2 * s) % n) for i in range(n)])


def swap_core(x):
    n = lax.axis_size("row")
    return lax.ppermute(x, "row", [(i, i ^ 1) for i in range(n)])


def at(x, k, dim=0):
    return lax.dynamic_index_in_dim(x, k, dim, keepdims=False)


def put(buf, x, k, dim=0):
    return lax.dynamic_update_slice_in_dim(buf, jnp.expand_dims(x, dim), k, dim)


def ring_gather(block, shift):
    half = block.shape[0] // 2
    back = shift(block, 1)
    front = shift(block, -1)
    far = (shift(back[:half], 1), shift(front[half:], -1))
    return ((0, block), (3, back), (1, front), (2, jnp.concatenate(far)))


def ring_exchange(piece, shift):
    far = piece(2)
    half = far.shape[0] // 2
    right, left = shift(far[:half], 1), shift(far[half:], -1)
    back = shift(piece(1), 1)
    front = shift(piece(3), -1)
    far = (shift(right, 1), shift(left, -1))
    return ((0, piece(0)), (3, back), (1, front), (2, jnp.concatenate(far)))


def ring_sum(parts, shift):
    f32 = jnp.float32
    halves = lax.optimization_barrier(jnp.split(parts, 8))
    far, ahead, behind, own = zip(halves[::2], halves[1::2])
    right, left = shift(far[0], 1), shift(far[1], -1)
    back_b = shift(ahead[1], 1)
    front_a = shift(behind[0], -1)
    back_a = shift(ahead[0] + right, 1)
    front_b = shift(behind[1] + left, -1)
    total = lambda a, b, c: a.astype(f32) + b.astype(f32) + c.astype(f32)
    return jnp.concatenate([total(own[0], back_a, front_a), total(own[1], back_b, front_b)])


def spread(x, axis):
    n = lax.axis_size(axis)
    return lax.all_to_all(jnp.broadcast_to(x[None], (n, *x.shape)), axis, 0, 0, tiled=True)


def logsum(values, dim):
    top = jnp.max(values, axis=dim)
    return top + jnp.log(jnp.sum(jnp.exp(values - jnp.expand_dims(top, dim)), axis=dim))


def ordered(core, own, other):
    return jnp.where(core == 0, jnp.stack([own, other]), jnp.stack([other, own]))


def local(hidden, embedding, teacher):
    f32, bf16 = jnp.float32, jnp.bfloat16
    layers, cols = lax.axis_size("layer"), lax.axis_size("col")
    rows = lax.axis_size("row")
    xs = rows // 2
    y, row = lax.axis_index("layer"), lax.axis_index("row")
    x, core = row // 2, row % 2
    strip, width = hidden.shape
    quarter = embedding.shape[1]
    block = embedding.shape[0] // layers
    half = strip * xs * layers

    moved = [shift_y(hidden, k) for k in (1, 3, 2)]
    mine = jnp.zeros((layers, strip, width), bf16)
    for k, p in ((0, hidden), (3, moved[0]), (1, moved[1]), (2, moved[2])):
        mine = put(mine, p, (y + k) % layers)

    table = embedding.T
    cut = lambda m, k: m[:, k * block : (k + 1) * block]
    sent = [jnp.concatenate([cut(table, k), cut(teacher, k)]) for k in range(layers)]
    sent = lax.all_to_all(jnp.stack(sent), "layer", 0, 0, tiled=True)
    table = sent[:, :quarter].reshape(width, block)
    taught = sent[:, quarter:].reshape(layers, xs, 2, strip, block)
    taught = [at(taught, c, 2).reshape(half, block) for c in (core, 1 - core)]

    own = jnp.zeros((layers, xs, strip, width), bf16)
    pieces = ring_gather(mine.reshape(layers * strip, width), shift_x)
    for k, p in pieces:
        own = put(own, p.reshape(layers, strip, width), (x + k) % xs, 1)
    own = own.reshape(half, width)
    other = swap_core(own)

    states = jnp.concatenate([own, other])
    logits = jnp.dot(states, table, preferred_element_type=f32)
    logits = with_layout_constraint(logits, Layout((0, 1)))
    lse_s = logsum(logits, 1)
    lse_s = ordered(core, lse_s[:half], lse_s[half:])
    lse_t = logsum(teacher.astype(f32), 1)
    got = spread(jnp.concatenate([lse_s.reshape(2 * half), lse_t]), ("layer", "row"))
    lse_s = logsum(got[:, : 2 * half], 0)
    lse_t = logsum(got[:, 2 * half :].reshape(layers, rows, -1), 1)
    got = spread(jnp.concatenate([lse_s, lse_t.reshape(2 * half)]), "col")
    lse_s, lse_t = jnp.split(logsum(got, 0), 2)
    lse_s = lse_s.reshape(2, half)
    lse_t = lse_t.reshape(layers * xs, 2, strip).swapaxes(0, 1).reshape(2, half)

    def gradient(logits, taught_c, c):
        taught_c = taught_c.astype(f32)
        prob_s = jnp.exp(logits - at(lse_s, c)[:, None])
        prob_t = jnp.exp(taught_c - at(lse_t, c)[:, None])
        return ((prob_s - prob_t) * LOSS_SCALE).astype(bf16)

    grads_other = gradient(logits[half:], taught[1], 1 - core)
    crossed = swap_core(grads_other)
    grads_own = gradient(logits[:half], taught[0], core)
    other_table = swap_core(table)


    both = jnp.concatenate([grads_own, crossed], axis=1)
    both = both.reshape(layers, xs, strip, 2 * block)
    tables = jnp.concatenate([table, other_table], axis=1)

    def part(*ks):
        picked = [at(both, (x + k) % xs, 1).reshape(layers * strip, 2 * block) for k in ks]
        return lax.dot_general(
            jnp.concatenate(picked), tables, (((1,), (1,)), ((), ())), preferred_element_type=f32
        ).astype(bf16)

    summed = ring_sum(part(2, 1, 3, 0), shift_x).astype(bf16)

    grads = jnp.concatenate([grads_own, grads_other])
    grad_table = lax.dot_general(
        states, grads, (((0,), (0,)), ((), ())), preferred_element_type=f32
    ).astype(bf16)
    grad_table = grad_table.reshape(layers, quarter, block)
    pieces = ring_exchange(lambda k: at(grad_table, (y + k) % layers), shift_y)
    grad_embedding = jnp.zeros((quarter, layers * block), f32)
    for k, p in pieces:
        grad_embedding = lax.dynamic_update_slice_in_dim(
            grad_embedding, p.astype(f32), ((y + k) % layers) * block, 1
        )

    share = strip // cols
    lanes = 128 if share * width % 128 == 0 else width
    summed = summed.reshape(layers * cols, share * width // lanes, lanes)
    summed = lax.all_to_all(summed, ("layer", "col"), 0, 0, tiled=True)
    grad_hidden = jnp.sum(summed.astype(f32), axis=0).reshape(share, width)
    return grad_embedding.T, grad_hidden


def solution(mesh):
    placed = (P(("layer", "row"), None), P(("row", "col"), "layer"), P("layer", ("row", "col")))
    return jax.shard_map(
        local,
        mesh=mesh,
        in_specs=placed,
        out_specs=(P(("row", "col"), "layer"), P(("layer", "row", "col"), None)),
        check_vma=False,
    )
```

```python
import jax
import jax.numpy as jnp
from jax import lax
from jax.experimental.layout import Layout, with_layout_constraint
from jax.sharding import PartitionSpec as P

LOSS_SCALE = 256


def shift_y(x, s):
    n = lax.axis_size("layer")
    return lax.ppermute(x, "layer", [(i, (i + s) % n) for i in range(n)])


def shift_x(x, s):
    n = lax.axis_size("row")
    return lax.ppermute(x, "row", [(i, (i + 2 * s) % n) for i in range(n)])


def swap_core(x):
    n = lax.axis_size("row")
    return lax.ppermute(x, "row", [(i, i ^ 1) for i in range(n)])


def at(x, k, dim=0):
    return lax.dynamic_index_in_dim(x, k, dim, keepdims=False)


def put(buf, x, k, dim=0):
    return lax.dynamic_update_slice_in_dim(buf, jnp.expand_dims(x, dim), k, dim)


def ring_gather(block, shift):
    half = block.shape[0] // 2
    back = shift(block, 1)
    front = shift(block, -1)
    far = (shift(back[:half], 1), shift(front[half:], -1))
    return ((0, block), (3, back), (1, front), (2, jnp.concatenate(far)))


def ring_exchange(piece, shift):
    far = piece(2)
    half = far.shape[0] // 2
    right, left = shift(far[:half], 1), shift(far[half:], -1)
    back = shift(piece(1), 1)
    front = shift(piece(3), -1)
    far = (shift(right, 1), shift(left, -1))
    return ((0, piece(0)), (3, back), (1, front), (2, jnp.concatenate(far)))


def ring_sum(parts, shift):
    f32 = jnp.float32
    halves = lax.optimization_barrier(jnp.split(parts, 8))
    far, ahead, behind, own = zip(halves[::2], halves[1::2])
    right, left = shift(far[0], 1), shift(far[1], -1)
    back_b = shift(ahead[1], 1)
    front_a = shift(behind[0], -1)
    back_a = shift(ahead[0] + right, 1)
    front_b = shift(behind[1] + left, -1)
    total = lambda a, b, c: a.astype(f32) + b.astype(f32) + c.astype(f32)
    return jnp.concatenate([total(own[0], back_a, front_a), total(own[1], back_b, front_b)])


def spread(x, axis):
    n = lax.axis_size(axis)
    return lax.all_to_all(jnp.broadcast_to(x[None], (n, *x.shape)), axis, 0, 0, tiled=True)


def logsum(values, dim):
    top = jnp.max(values, axis=dim)
    return top + jnp.log(jnp.sum(jnp.exp(values - jnp.expand_dims(top, dim)), axis=dim))


def ordered(core, own, other):
    return jnp.where(core == 0, jnp.stack([own, other]), jnp.stack([other, own]))


def local(hidden, embedding, teacher):
    f32, bf16 = jnp.float32, jnp.bfloat16
    layers, cols = lax.axis_size("layer"), lax.axis_size("col")
    rows = lax.axis_size("row")
    xs = rows // 2
    y, row = lax.axis_index("layer"), lax.axis_index("row")
    x, core = row // 2, row % 2
    strip, width = hidden.shape
    quarter = embedding.shape[1]
    block = embedding.shape[0] // layers
    half = strip * xs * layers

    moved = [shift_y(hidden, k) for k in (1, 3, 2)]
    mine = jnp.zeros((layers, strip, width), bf16)
    for k, p in ((0, hidden), (3, moved[0]), (1, moved[1]), (2, moved[2])):
        mine = put(mine, p, (y + k) % layers)

    cut = lambda m: jnp.stack([m[:, k * block : (k + 1) * block] for k in range(layers)])
    table = lax.all_to_all(cut(embedding.T), "layer", 0, 0, tiled=True)
    table = table.reshape(width, block)
    taught = lax.all_to_all(cut(teacher), "layer", 0, 0, tiled=True)
    taught = taught.reshape(layers, xs, 2, strip, block)
    taught = [at(taught, c, 2).reshape(half, block) for c in (core, 1 - core)]

    own = jnp.zeros((layers, xs, strip, width), bf16)
    pieces = ring_gather(mine.reshape(layers * strip, width), shift_x)
    for k, p in pieces:
        own = put(own, p.reshape(layers, strip, width), (x + k) % xs, 1)
    own = own.reshape(half, width)
    other = swap_core(own)

    states = jnp.concatenate([own, other])
    logits = jnp.dot(states, table, preferred_element_type=f32)
    logits = with_layout_constraint(logits, Layout((0, 1)))
    lse_s = logsum(logits, 1)
    lse_s = ordered(core, lse_s[:half], lse_s[half:])
    lse_t = logsum(teacher.astype(f32), 1)
    got = spread(jnp.concatenate([lse_s.reshape(2 * half), lse_t]), ("layer", "row"))
    lse_s = logsum(got[:, : 2 * half], 0)
    lse_t = logsum(got[:, 2 * half :].reshape(layers, rows, -1), 1)
    got = spread(jnp.concatenate([lse_s, lse_t.reshape(2 * half)]), "col")
    lse_s, lse_t = jnp.split(logsum(got, 0), 2)
    lse_s = lse_s.reshape(2, half)
    lse_t = lse_t.reshape(layers * xs, 2, strip).swapaxes(0, 1).reshape(2, half)

    def gradient(logits, taught_c, c):
        taught_c = taught_c.astype(f32)
        prob_s = jnp.exp(logits - at(lse_s, c)[:, None])
        prob_t = jnp.exp(taught_c - at(lse_t, c)[:, None])
        return ((prob_s - prob_t) * LOSS_SCALE).astype(bf16)

    grads_other = gradient(logits[half:], taught[1], 1 - core)
    crossed = swap_core(grads_other)
    logits_own, grads_other = lax.optimization_barrier((logits[:half], grads_other))
    grads_own = gradient(logits_own, taught[0], core)
    other_table = swap_core(table)


    both = jnp.concatenate([grads_own, crossed], axis=1)
    both = both.reshape(layers, xs, strip, 2 * block)
    tables = jnp.concatenate([table, other_table], axis=1)

    def part(*ks):
        picked = [at(both, (x + k) % xs, 1).reshape(layers * strip, 2 * block) for k in ks]
        return lax.dot_general(
            jnp.concatenate(picked), tables, (((1,), (1,)), ((), ())), preferred_element_type=f32
        ).astype(bf16)

    summed = ring_sum(part(2, 1, 3, 0), shift_x).astype(bf16)

    grads = jnp.concatenate([grads_own, grads_other])
    grad_table = lax.dot_general(
        states, grads, (((0,), (0,)), ((), ())), preferred_element_type=f32
    ).astype(bf16)
    grad_table = grad_table.reshape(layers, quarter, block)
    pieces = ring_exchange(lambda k: at(grad_table, (y + k) % layers), shift_y)
    grad_embedding = jnp.zeros((quarter, layers * block), f32)
    for k, p in pieces:
        grad_embedding = lax.dynamic_update_slice_in_dim(
            grad_embedding, p.astype(f32), ((y + k) % layers) * block, 1
        )

    share = strip // cols
    lanes = 128 if share * width % 128 == 0 else width
    summed = summed.reshape(layers * cols, share * width // lanes, lanes)
    summed = lax.all_to_all(summed, ("layer", "col"), 0, 0, tiled=True)
    grad_hidden = jnp.sum(summed.astype(f32), axis=0).reshape(share, width)
    return grad_embedding.T, grad_hidden


def solution(mesh):
    placed = (P(("layer", "row"), None), P(("row", "col"), "layer"), P("layer", ("row", "col")))
    return jax.shard_map(
        local,
        mesh=mesh,
        in_specs=placed,
        out_specs=(P(("row", "col"), "layer"), P(("layer", "row", "col"), None)),
        check_vma=False,
    )
```

```python
import jax
import jax.numpy as jnp
from jax import lax
from jax.experimental.layout import Layout, with_layout_constraint
from jax.sharding import PartitionSpec as P

LOSS_SCALE = 256


def shift_y(x, s):
    n = lax.axis_size("layer")
    return lax.ppermute(x, "layer", [(i, (i + s) % n) for i in range(n)])


def shift_x(x, s):
    n = lax.axis_size("row")
    return lax.ppermute(x, "row", [(i, (i + 2 * s) % n) for i in range(n)])


def swap_core(x):
    n = lax.axis_size("row")
    return lax.ppermute(x, "row", [(i, i ^ 1) for i in range(n)])


def at(x, k, dim=0):
    return lax.dynamic_index_in_dim(x, k, dim, keepdims=False)


def put(buf, x, k, dim=0):
    return lax.dynamic_update_slice_in_dim(buf, jnp.expand_dims(x, dim), k, dim)


def ring_gather(block, shift):
    half = block.shape[0] // 2
    back = shift(block, 1)
    front = shift(block, -1)
    far = (shift(back[:half], 1), shift(front[half:], -1))
    return ((0, block), (3, back), (1, front), (2, jnp.concatenate(far)))


def ring_exchange(piece, shift):
    far = piece(2)
    half = far.shape[0] // 2
    right, left = shift(far[:half], 1), shift(far[half:], -1)
    back = shift(piece(1), 1)
    front = shift(piece(3), -1)
    far = (shift(right, 1), shift(left, -1))
    return ((0, piece(0)), (3, back), (1, front), (2, jnp.concatenate(far)))


def ring_sum(part, shift):
    f32 = jnp.float32
    far = lax.optimization_barrier(jnp.split(part(2), 2))
    rest = part(1, 3, 0)
    halves = lax.optimization_barrier(jnp.split(rest, 6))
    ahead, behind, own = zip(halves[::2], halves[1::2])
    right, left = shift(far[0], 1), shift(far[1], -1)
    back_b = shift(ahead[1], 1)
    front_a = shift(behind[0], -1)
    back_a = shift(ahead[0] + right, 1)
    front_b = shift(behind[1] + left, -1)
    total = lambda a, b, c: a.astype(f32) + b.astype(f32) + c.astype(f32)
    return jnp.concatenate([total(own[0], back_a, front_a), total(own[1], back_b, front_b)])


def spread(x, axis):
    n = lax.axis_size(axis)
    return lax.all_to_all(jnp.broadcast_to(x[None], (n, *x.shape)), axis, 0, 0, tiled=True)


def logsum(values, dim):
    top = jnp.max(values, axis=dim)
    return top + jnp.log(jnp.sum(jnp.exp(values - jnp.expand_dims(top, dim)), axis=dim))


def ordered(core, own, other):
    return jnp.where(core == 0, jnp.stack([own, other]), jnp.stack([other, own]))


def local(hidden, embedding, teacher):
    f32, bf16 = jnp.float32, jnp.bfloat16
    layers, cols = lax.axis_size("layer"), lax.axis_size("col")
    rows = lax.axis_size("row")
    xs = rows // 2
    y, row = lax.axis_index("layer"), lax.axis_index("row")
    x, core = row // 2, row % 2
    strip, width = hidden.shape
    quarter = embedding.shape[1]
    block = embedding.shape[0] // layers
    half = strip * xs * layers

    moved = [shift_y(hidden, k) for k in (1, 3, 2)]
    mine = jnp.zeros((layers, strip, width), bf16)
    for k, p in ((0, hidden), (3, moved[0]), (1, moved[1]), (2, moved[2])):
        mine = put(mine, p, (y + k) % layers)

    cut = lambda m: jnp.stack([m[:, k * block : (k + 1) * block] for k in range(layers)])
    table = lax.all_to_all(cut(embedding.T), "layer", 0, 0, tiled=True)
    table = table.reshape(width, block)
    taught = lax.all_to_all(cut(teacher), "layer", 0, 0, tiled=True)
    taught = taught.reshape(layers, xs, 2, strip, block)
    taught = [at(taught, c, 2).reshape(half, block) for c in (core, 1 - core)]

    own = jnp.zeros((layers, xs, strip, width), bf16)
    pieces = ring_gather(mine.reshape(layers * strip, width), shift_x)
    for k, p in pieces:
        own = put(own, p.reshape(layers, strip, width), (x + k) % xs, 1)
    own = own.reshape(half, width)
    other = swap_core(own)

    def scores(states):
        logits = jnp.dot(states, table, preferred_element_type=f32)
        return with_layout_constraint(logits, Layout((0, 1)))

    logits_own = scores(own)
    logits_other = scores(other)
    lse_s = ordered(core, logsum(logits_own, 1), logsum(logits_other, 1))
    lse_t = logsum(teacher.astype(f32), 1)
    got = spread(jnp.concatenate([lse_s.reshape(2 * half), lse_t]), ("layer", "row"))
    lse_s = logsum(got[:, : 2 * half], 0)
    lse_t = logsum(got[:, 2 * half :].reshape(layers, rows, -1), 1)
    got = spread(jnp.concatenate([lse_s, lse_t.reshape(2 * half)]), "col")
    lse_s, lse_t = jnp.split(logsum(got, 0), 2)
    lse_s = lse_s.reshape(2, half)
    lse_t = lse_t.reshape(layers * xs, 2, strip).swapaxes(0, 1).reshape(2, half)

    def gradient(logits, taught_c, c):
        taught_c = taught_c.astype(f32)
        prob_s = jnp.exp(logits - at(lse_s, c)[:, None])
        prob_t = jnp.exp(taught_c - at(lse_t, c)[:, None])
        return ((prob_s - prob_t) * LOSS_SCALE).astype(bf16)

    grads_other = gradient(logits_other, taught[1], 1 - core)
    crossed = swap_core(grads_other)
    logits_own, grads_other = lax.optimization_barrier((logits_own, grads_other))
    grads_own = gradient(logits_own, taught[0], core)
    other_table = swap_core(table)


    both = jnp.concatenate([grads_own, crossed], axis=1)
    both = both.reshape(layers, xs, strip, 2 * block)
    tables = jnp.concatenate([table, other_table], axis=1)

    def part(*ks):
        picked = [at(both, (x + k) % xs, 1).reshape(layers * strip, 2 * block) for k in ks]
        return lax.dot_general(
            jnp.concatenate(picked), tables, (((1,), (1,)), ((), ())), preferred_element_type=f32
        ).astype(bf16)

    summed = ring_sum(part, shift_x).astype(bf16)

    grads = jnp.concatenate([grads_own, grads_other])
    grad_table = lax.dot_general(
        jnp.concatenate([own, other]), grads, (((0,), (0,)), ((), ())),
        preferred_element_type=f32,
    ).astype(bf16)
    grad_table = grad_table.reshape(layers, quarter, block)
    pieces = ring_exchange(lambda k: at(grad_table, (y + k) % layers), shift_y)
    grad_embedding = jnp.zeros((quarter, layers * block), f32)
    for k, p in pieces:
        grad_embedding = lax.dynamic_update_slice_in_dim(
            grad_embedding, p.astype(f32), ((y + k) % layers) * block, 1
        )

    share = strip // cols
    lanes = 128 if share * width % 128 == 0 else width
    summed = summed.reshape(layers * cols, share * width // lanes, lanes)
    summed = lax.all_to_all(summed, ("layer", "col"), 0, 0, tiled=True)
    grad_hidden = jnp.sum(summed.astype(f32), axis=0).reshape(share, width)
    return grad_embedding.T, grad_hidden


def solution(mesh):
    placed = (P(("layer", "row"), None), P(("row", "col"), "layer"), P("layer", ("row", "col")))
    return jax.shard_map(
        local,
        mesh=mesh,
        in_specs=placed,
        out_specs=(P(("row", "col"), "layer"), P(("layer", "row", "col"), None)),
        check_vma=False,
    )
```
